32 devices in a mesh: grid: 8 (over y, x, core), band: 4 (over z).
Axes of the slice: x: 2, y: 2, z: 4, core: 2. Of those that a mesh axis runs over, the one named last changes fastest.
Arguments:
- start: float32 [1, 4, 1, 64, 32768], P(None, None, None, 'band', 'grid'), may hold values from -6 to 6
- energies: float32 [4, 64, 32768], P(None, 'band', 'grid'), may hold values from -4 to 4
- sites: int32 [3, 1], replicated, may hold values from 0 to 31
- potential: float32 [32, 32, 32], replicated, may hold values from -4 to 400
Outputs:
- alphas: float32 [1, 1, 4], replicated
- betas: float32 [1, 1, 4], replicated
- lanczos: float32 [1, 4, 1, 64, 32768], P(None, None, None, 'band', 'grid')
The draws below stay inside these ranges and needn't reach their ends.
All inputs are finite; a program needn't handle non-finite values.
Results may differ from the reference program's by a relative error of at most 0.0003.
Values sent between devices are 32-bit elements; how exact they have to be, the bound alone decides.
No kernel may reach another device: no remote copies, remote signals or barrier semaphores. Data moves between devices by JAX's collectives and lax.ppermute only.
A program may use at most 64 MiB of HBM per device.

```python
import jax
import jax.numpy as jnp
from jax import lax

GRIDN = 32
CBANDS = 64
CORES = 4
POLS = 1
ITERS = 4
ATOMS = 1
KPOINTS = 32768


def draw_potential(key, part):
    first, second = jax.random.split(key)
    coords = jnp.arange(GRIDN, dtype=jnp.int32)
    distance = jnp.minimum(coords, GRIDN - coords).astype(jnp.float32)
    square = distance[:, None, None] ** 2 + distance[None, :, None] ** 2 + distance[None, None, :] ** 2
    radius = jnp.sqrt(square)
    spread_cells, height, tail_charge, background = (1.5, 250.0, 6.0, 3.0)
    roughness = jax.random.uniform(first, (GRIDN, GRIDN, GRIDN), jnp.float32, 0.5, 1.5)
    jitter = jax.random.uniform(second, (GRIDN, GRIDN, GRIDN), jnp.float32, -1.0, 1.0)
    peaked = height * jnp.exp(-square / (2.0 * spread_cells * spread_cells)) * roughness
    screened_tail = tail_charge / jnp.maximum(radius, 0.5)
    return peaked + screened_tail + background * jitter


def block_scale(rng, extent, shards, least, top_value):
    def one(position, parts):
        steps = jax.random.uniform(jax.random.fold_in(jax.random.fold_in(rng, 6), position), (parts,), jnp.float32, least / len(shards), top_value / len(shards))
        return jnp.repeat(jnp.exp(steps), extent[position] // parts).reshape((-1,) + (1,) * (len(extent) - position - 1))

    gain = one(*shards[0])
    for cut in shards[1:]:
        gain = gain * one(*cut)
    return gain


def scatter_about(key, extent, spread, reach, pieces=(), kind=jnp.bfloat16):
    array = spread * jax.random.normal(key, extent, jnp.float32)
    if pieces:
        array = array * block_scale(key, extent, pieces, -0.22, 0.18)
    return jnp.clip(array, -reach, reach).astype(kind)


def setup_inputs(seed: int = 0) -> dict:
    splits = jax.random.split(jax.random.key(seed), 5)
    start = scatter_about(splits[0], (ATOMS, CORES, POLS, CBANDS, KPOINTS), 1.0, 6.0, ((3, 4), (4, 8)), jnp.float32)
    energies = jnp.clip(jax.random.uniform(splits[1], (CORES, CBANDS, KPOINTS), jnp.float32, -4.0, 4.0) * block_scale(splits[1], (CORES, CBANDS, KPOINTS), ((1, 4), (2, 8)), -0.4, 0.0), -4.0, 4.0)
    sites = jax.random.randint(splits[2], (3, ATOMS), 0, GRIDN).astype(jnp.int32)
    potential = draw_potential(jax.random.fold_in(splits[4], 71), 0)
    return dict(start=start, energies=energies, sites=sites, potential=potential)


def cas_along(field_part, axis_number):
    spectrum = jnp.fft.fft(field_part, axis=axis_number)
    return (spectrum.real - spectrum.imag).astype(field_part.dtype)

def cas_three(field_part):
    return cas_along(cas_along(cas_along(field_part, 1), 2), 3)

def shift_axis(field_part, offset, axis_number):
    length = field_part.shape[axis_number]
    doubled = jnp.concatenate([field_part, field_part], axis=axis_number)
    first_index = ((length - offset) % length).astype(jnp.int32)
    return lax.dynamic_slice_in_dim(doubled, first_index, length, axis_number)

def reference(start, energies, sites, potential):
    grid_size = potential.shape[0]
    volume = grid_size * grid_size * grid_size
    shifted_list = []
    for atom_index in range(ATOMS):
        shifted = shift_axis(potential, sites[0, atom_index], 0)
        shifted = shift_axis(shifted, sites[1, atom_index], 1)
        shifted = shift_axis(shifted, sites[2, atom_index], 2)
        shifted_list.append(shifted)
    weights_all = jnp.repeat(jnp.stack(shifted_list), CORES, axis=0)

    def per_block(pair_items):
        field_block, weights = pair_items
        return cas_three(weights[None] * cas_three(field_block)) / volume

    def direct(vector):
        flat_vec = vector.reshape(ATOMS * CORES, POLS * CBANDS, grid_size, grid_size, grid_size)
        result = lax.map(per_block, (flat_vec, weights_all))
        return result.reshape(vector.shape)
    total_count = CORES * CBANDS * KPOINTS

    def inner(left, right):
        return lax.optimization_barrier(jnp.sum(left * right, axis=(1, 3, 4))) / total_count

    def expand_coef(values):
        return values[:, None, :, None, None]
    lanczos = start / expand_coef(jnp.sqrt(inner(start, start)))
    previous = jnp.zeros_like(start)
    beta_prev = jnp.zeros((ATOMS, POLS), jnp.float32)
    alpha_list = []
    beta_list = []
    for iteration in range(ITERS):
        applied = energies[None, :, None] * lanczos - direct(lanczos)
        alpha_now = inner(lanczos, applied)
        remainder = applied - expand_coef(alpha_now) * lanczos - expand_coef(beta_prev) * previous
        beta_now = jnp.sqrt(inner(remainder, remainder))
        previous = lanczos
        lanczos = remainder / expand_coef(beta_now)
        beta_prev = beta_now
        alpha_list.append(alpha_now)
        beta_list.append(beta_now)
    return (jnp.stack(alpha_list, axis=2), jnp.stack(beta_list, axis=2), lanczos)
```

```python
import functools
import math

import jax
import jax.numpy as jnp
import numpy as np
from jax import lax
from jax.experimental import pallas as pl
from jax.experimental.pallas import tpu as pltpu
from jax.sharding import PartitionSpec as P

ITERS = 4
LANES = 128
RADIX = 8
PAIRS = 4
RESIDUES = ((0, 4), (1, 7), (2, 6), (3, 5))
HALF_ROOT = math.sqrt(0.5)
ROW_BETA = 8
ROW_NORM = 16
ROW_LAST = 17
ROWS = 24


def cas(angle):
    return np.cos(angle) + np.sin(angle)


@functools.cache
def pair_weights(size):
    low = size // RADIX
    cells = np.arange(size)
    over_z = cas(2 * np.pi * np.outer(cells, cells) / size)
    weights = np.zeros((PAIRS, 2, low, size, 2, low, size))
    for pair, residues in enumerate(RESIDUES):
        for out_half, residue in enumerate(residues):
            for v0 in range(low):
                for y0 in range(low):
                    angle = 2 * np.pi * (residue + RADIX * v0) * y0 / size
                    cosine, sine = np.cos(angle), np.sin(angle)
                    if pair == 0:
                        weights[pair, out_half, y0, :, out_half, v0] = (cosine + sine) * over_z
                    else:
                        sign = 1.0 if out_half == 0 else -1.0
                        weights[pair, 0, y0, :, out_half, v0] = (cosine + sine) * over_z
                        weights[pair, 1, y0, :, out_half, v0] = sign * (cosine - sine) * over_z
    return weights.reshape(PAIRS, 2 * low * size, 2 * low * size)


def split_weights(weights):
    high = weights.astype(np.float32).astype(jnp.bfloat16)
    rest = (weights - high.astype(np.float64)).astype(np.float32).astype(jnp.bfloat16)
    return high, rest


def hartley(values):
    count = len(values)
    if count == 2:
        return [values[0] + values[1], values[0] - values[1]]
    even, odd = hartley(values[0::2]), hartley(values[1::2])
    half = count // 2
    first, second = [], []
    for u in range(half):
        angle = 2 * math.pi * u / count
        if u == 0:
            turned = odd[0]
        elif 4 * u == count:
            turned = odd[u]
        elif 8 * u == count:
            turned = (odd[u] + odd[half - u]) * HALF_ROOT
        elif 8 * u == 3 * count:
            turned = (odd[half - u] - odd[u]) * HALF_ROOT
        else:
            turned = odd[u] * math.cos(angle) + odd[half - u] * math.sin(angle)
        first.append(even[u] + turned)
        second.append(even[u] - turned)
    return first + second


def butterflies(f):
    a = [f[i] + f[i + 4] for i in range(4)]
    b = [f[i] - f[i + 4] for i in range(4)]
    even, odd = a[0] + a[2], a[1] + a[3]
    less, more = (b[1] - b[3]) * HALF_ROOT, (b[1] + b[3]) * HALF_ROOT
    return (
        (even + odd, even - odd),
        (b[0] + less, b[2] + more),
        (a[0] - a[2], a[1] - a[3]),
        (b[0] - less, more - b[2]),
    )


def butterflies_back(pairs):
    (c0, c4), (c1, s1), (c2, s2), (c3, s3) = pairs
    even, odd = c0 + c4, c0 - c4
    less, more = (c1 - c3) * HALF_ROOT, (s1 + s3) * HALF_ROOT
    a = [even + c2, odd + s2, even - c2, odd - s2]
    b = [c1 + c3, less + more, s1 - s3, more - less]
    return [a[i] + b[i] for i in range(4)] + [a[i] - b[i] for i in range(4)]


def total(block):
    return jnp.sum(jnp.sum(block, axis=0, keepdims=True), axis=1, keepdims=True)


def guarded(square):
    root = jnp.sqrt(square)
    positive = root > 0.0
    return root, jnp.where(positive, 1.0 / jnp.where(positive, root, 1.0), 0.0)


def matmul3(value, high_ref, rest_ref, pair):
    high = value.astype(jnp.bfloat16)
    rest = (value - high.astype(jnp.float32)).astype(jnp.bfloat16)
    dot = functools.partial(jnp.dot, preferred_element_type=jnp.float32)
    return dot(high, high_ref[pair]) + (dot(rest, high_ref[pair]) + dot(high, rest_ref[pair]))


def recur_kernel(
    size, both_ref, pot_ref, fwd_high, fwd_rest, back_high, back_rest,
    basis_ref, message_ref, own_ref, left, right,
):
    groups, double, width = both_ref.shape
    fields = double // 2
    planes = width // (size * size)

    def rows_of(group, plane):
        return pl.ds(pl.multiple_of((group * planes + plane) * fields, 8), fields)

    def cut(plane, block):
        start = (plane * RADIX + block) * LANES
        return slice(start, start + LANES)

    def over_planes(step, init):
        def run(group, carry):
            for plane in range(planes):
                carry = step(group, plane, carry)
            return carry

        return lax.fori_loop(0, groups, run, init)

    zero = jnp.zeros((fields, LANES), jnp.float32)

    def take_start(group, plane, carry):
        for block in range(RADIX):
            value = both_ref[group, :fields, cut(plane, block)]
            basis_ref[0, group, :, cut(plane, block)] = value
            carry = carry + value * value
        return carry

    norm, scale = guarded(total(over_planes(take_start, zero)))
    row = lax.broadcasted_iota(jnp.int32, (ROWS, LANES), 0)
    stats = jnp.where(row == ROW_NORM, norm, 0.0)

    def iteration(step, state):
        stats, scale, beta_prev = state
        before = jnp.maximum(step - 1, 0)

        def forward(group, plane, carry):
            values = []
            for block in range(RADIX):
                value = basis_ref[step, group, :, cut(plane, block)] * scale
                basis_ref[step, group, :, cut(plane, block)] = value
                values.append(value)
            for pair, halves in enumerate(butterflies(values)):
                for half, value in enumerate(halves):
                    left[pair, rows_of(group, plane), half * LANES : (half + 1) * LANES] = value
            return carry

        over_planes(forward, 0)

        def middle(pair, carry):
            right[pair] = matmul3(left[pair], fwd_high, fwd_rest, pair)
            for half in range(2):
                lanes = slice(half * LANES, (half + 1) * LANES)
                column = [right[pair, x * fields : (x + 1) * fields, lanes] for x in range(size)]
                column = hartley(column)
                column = [column[x] * pot_ref[pair, x : x + 1, lanes] for x in range(size)]
                column = hartley(column)
                for x in range(size):
                    left[pair, x * fields : (x + 1) * fields, lanes] = column[x]
            right[pair] = matmul3(left[pair], back_high, back_rest, pair)
            return carry

        lax.fori_loop(0, PAIRS, middle, 0)

        def backward(group, plane, carry):
            pairs = []
            for pair in range(PAIRS):
                pairs.append(
                    [
                        right[pair, rows_of(group, plane), half * LANES : (half + 1) * LANES]
                        for half in range(2)
                    ]
                )
            for block, direct in enumerate(butterflies_back(pairs)):
                place = cut(plane, block)
                value = basis_ref[step, group, :, place]
                applied = both_ref[group, fields:, place] * value - direct
                applied = applied - beta_prev * basis_ref[before, group, :, place]
                basis_ref[step + 1, group, :, place] = applied
                carry = carry + value * applied
            return carry

        alpha = total(over_planes(backward, zero))

        def remove(group, plane, carry):
            for block in range(RADIX):
                place = cut(plane, block)
                value = basis_ref[step + 1, group, :, place]
                value = value - alpha * basis_ref[step, group, :, place]
                basis_ref[step + 1, group, :, place] = value
                carry = carry + value * value
            return carry

        beta, scale = guarded(total(over_planes(remove, zero)))
        stats = jnp.where(row == step, alpha, stats)
        stats = jnp.where(row == step + ROW_BETA, beta, stats)
        return jnp.where(row == ROW_LAST, scale, stats), scale, beta

    one = jnp.zeros((1, 1), jnp.float32)
    stats, _, _ = lax.fori_loop(0, ITERS, iteration, (stats, scale, one))
    own_ref[...] = stats
    lane = lax.broadcasted_iota(jnp.int32, (1, LANES), 1)
    message = jnp.zeros((1, LANES), jnp.float32)
    for place in [*range(ITERS), *range(ROW_BETA, ROW_BETA + ITERS), ROW_NORM]:
        message = jnp.where(lane == place, stats[place : place + 1], message)
    message_ref[...] = jnp.broadcast_to(message[None], message_ref.shape)


def combine_kernel(
    root_count, planes, all_ref, own_ref, basis_ref, result_ref, alpha_ref, beta_ref
):
    groups, fields, width = result_ref.shape
    table = jnp.transpose(all_ref[:, 0, :])
    wide_alpha, wide_beta = table[0:8], table[8:16]
    own_alpha, own_beta = own_ref[0:8], own_ref[8:16]
    square = table[ROW_NORM : ROW_NORM + 1]
    _, inverse = guarded(total(square * square))

    def first(norm, like):
        row = lax.broadcasted_iota(jnp.int32, like.shape, 0)
        return jnp.where(row == 0, norm * inverse, 0.0)

    def apply(diagonal, side, vector):
        return diagonal * vector + side * pltpu.roll(vector, 7, 0) + pltpu.roll(side * vector, 1, 0)

    wide = first(square, wide_alpha)
    own = first(own_ref[ROW_NORM : ROW_NORM + 1], own_alpha)
    wide_prev, own_prev = jnp.zeros_like(wide), jnp.zeros_like(own)
    beta = jnp.zeros((1, 1), jnp.float32)
    lane = lax.broadcasted_iota(jnp.int32, (1, LANES), 1)
    alphas = jnp.zeros((1, LANES), jnp.float32)
    betas = jnp.zeros((1, LANES), jnp.float32)
    for step in range(ITERS):
        applied = apply(wide_alpha, wide_beta, wide)
        alpha = total(wide * applied)
        remainder = applied - alpha * wide - beta * wide_prev
        own_remainder = apply(own_alpha, own_beta, own) - alpha * own - beta * own_prev
        beta = jnp.sqrt(total(remainder * remainder))
        wide_prev, own_prev = wide, own
        wide, own = remainder / beta, own_remainder / beta
        alphas = jnp.where(lane == step, alpha, alphas)
        betas = jnp.where(lane == step, beta, betas)
    alpha_ref[0] = alphas[:, :ITERS]
    beta_ref[0] = betas[:, :ITERS]
    factors = [own[i : i + 1] * root_count for i in range(ITERS + 1)]
    factors[ITERS] = factors[ITERS] * own_ref[ROW_LAST : ROW_LAST + 1]

    def run(group, carry):
        for block in range(width // LANES):
            place = slice(block * LANES, (block + 1) * LANES)
            value = basis_ref[0, group, :, place] * factors[0]
            for i in range(1, ITERS + 1):
                value = value + basis_ref[i, group, :, place] * factors[i]
            result_ref[group, :, place] = value
        return carry

    lax.fori_loop(0, groups, run, 0)


def shift_axis(part, offset, axis_number):
    length = part.shape[axis_number]
    doubled = jnp.concatenate([part, part], axis=axis_number)
    first_index = (length - offset) % length
    return lax.dynamic_slice_in_dim(doubled, first_index, length, axis_number)


def potential_table(potential, sites):
    size = potential.shape[0]
    table = potential
    for axis in range(3):
        table = shift_axis(table, sites[axis, 0], axis)
    table = table * (1.0 / size**3)
    table = table.reshape(size, size // RADIX, RADIX, size)
    pairs = [
        jnp.concatenate([table[:, :, residue].reshape(size, -1) for residue in residues], axis=1)
        for residues in RESIDUES
    ]
    return jnp.stack(pairs)


def body(start, energies, sites, potential):
    size = potential.shape[0]
    atom_count, core_count, pol_count, band_local, kpoint_local = start.shape
    assert atom_count == 1 and pol_count == 1 and size * (size // RADIX) == LANES
    groups = lax.axis_size("grid")
    devices = groups * lax.axis_size("band")
    chain = core_count * band_local
    planes = size // groups
    fields = -(-chain // groups)
    padded = -(-fields // 8) * 8

    def by_owner(part):
        part = part.reshape(chain, kpoint_local)
        if fields * groups != chain:
            part = jnp.pad(part, ((0, fields * groups - chain), (0, 0)))
        part = part.reshape(groups, fields, kpoint_local)
        if padded != fields:
            part = jnp.pad(part, ((0, 0), (0, padded - fields), (0, 0)))
        return part

    both = jnp.concatenate([by_owner(start), by_owner(energies)], axis=1)
    both = lax.all_to_all(both, "grid", split_axis=0, concat_axis=0, tiled=True)
    table = potential_table(potential, sites)
    weights = pair_weights(size)
    fwd_high, fwd_rest = split_weights(weights)
    back_high, back_rest = split_weights(weights.transpose(0, 2, 1))
    vmem = pl.BlockSpec(memory_space=pltpu.VMEM)
    shape = functools.partial(jax.ShapeDtypeStruct, dtype=jnp.float32)
    pair_shape = (PAIRS, size * padded, 2 * LANES)
    basis, message, own = pl.pallas_call(
        functools.partial(recur_kernel, size),
        out_shape=(
            shape((ITERS + 1, groups, padded, kpoint_local)),
            shape((devices, 1, LANES)),
            shape((ROWS, LANES)),
        ),
        in_specs=[vmem] * 6,
        out_specs=(vmem, vmem, vmem),
        scratch_shapes=[pltpu.VMEM(pair_shape, jnp.float32)] * 2,
        compiler_params=pltpu.CompilerParams(vmem_limit_bytes=24 * 2**20),
        name="recur",
    )(both, table, *map(jnp.asarray, (fwd_high, fwd_rest, back_high, back_rest)))
    gathered = lax.all_to_all(message, ("grid", "band"), split_axis=0, concat_axis=0, tiled=True)
    count = chain * lax.axis_size("band") * kpoint_local * groups
    result, alphas, betas = pl.pallas_call(
        functools.partial(combine_kernel, math.sqrt(count), planes),
        out_shape=(
            shape((groups, padded, kpoint_local)),
            shape((1, 1, ITERS)),
            shape((1, 1, ITERS)),
        ),
        in_specs=[vmem] * 3,
        out_specs=(vmem, vmem, vmem),
        compiler_params=pltpu.CompilerParams(vmem_limit_bytes=16 * 2**20),
        name="combine",
    )(gathered, own, basis)
    back = lax.all_to_all(result, "grid", split_axis=0, concat_axis=0, tiled=True)
    back = back[:, :fields].reshape(groups * fields, kpoint_local)[:chain]
    return alphas, betas, back.reshape(start.shape)


def solution(mesh):
    in_specs = (P(None, None, None, "band", "grid"), P(None, "band", "grid"), P(), P())
    out_specs = (P(), P(), P(None, None, None, "band", "grid"))
    return jax.shard_map(body, mesh=mesh, in_specs=in_specs, out_specs=out_specs, check_vma=False)
```

```python
import functools
import math

import jax
import jax.numpy as jnp
import numpy as np
from jax import lax
from jax.experimental import pallas as pl
from jax.experimental.pallas import tpu as pltpu
from jax.sharding import PartitionSpec as P

ITERS = 4
LANES = 128
RADIX = 8
PAIRS = 4
RESIDUES = ((0, 4), (1, 7), (2, 6), (3, 5))
HALF_ROOT = math.sqrt(0.5)
ROW_BETA = 8
ROW_NORM = 16
ROW_INVERSE = 17
ROWS = 24


def cas(angle):
    return np.cos(angle) + np.sin(angle)


@functools.cache
def pair_weights(size):
    low = size // RADIX
    cells = np.arange(size)
    over_z = cas(2 * np.pi * np.outer(cells, cells) / size)
    weights = np.zeros((PAIRS, 2, low, size, 2, low, size))
    for pair, residues in enumerate(RESIDUES):
        for out_half, residue in enumerate(residues):
            for v0 in range(low):
                for y0 in range(low):
                    angle = 2 * np.pi * (residue + RADIX * v0) * y0 / size
                    cosine, sine = np.cos(angle), np.sin(angle)
                    if pair == 0:
                        weights[pair, out_half, y0, :, out_half, v0] = (cosine + sine) * over_z
                    else:
                        sign = 1.0 if out_half == 0 else -1.0
                        weights[pair, 0, y0, :, out_half, v0] = (cosine + sine) * over_z
                        weights[pair, 1, y0, :, out_half, v0] = sign * (cosine - sine) * over_z
    return weights.reshape(PAIRS, 2 * low * size, 2 * low * size)


def split_weights(weights):
    high = weights.astype(np.float32).astype(jnp.bfloat16)
    rest = (weights - high.astype(np.float64)).astype(np.float32).astype(jnp.bfloat16)
    return high, rest


def hartley(values):
    count = len(values)
    if count == 2:
        return [values[0] + values[1], values[0] - values[1]]
    even, odd = hartley(values[0::2]), hartley(values[1::2])
    half = count // 2
    first, second = [], []
    for u in range(half):
        angle = 2 * math.pi * u / count
        if u == 0:
            turned = odd[0]
        elif 4 * u == count:
            turned = odd[u]
        elif 8 * u == count:
            turned = (odd[u] + odd[half - u]) * HALF_ROOT
        elif 8 * u == 3 * count:
            turned = (odd[half - u] - odd[u]) * HALF_ROOT
        else:
            turned = odd[u] * math.cos(angle) + odd[half - u] * math.sin(angle)
        first.append(even[u] + turned)
        second.append(even[u] - turned)
    return first + second


def butterflies(f):
    a = [f[i] + f[i + 4] for i in range(4)]
    b = [f[i] - f[i + 4] for i in range(4)]
    even, odd = a[0] + a[2], a[1] + a[3]
    less, more = (b[1] - b[3]) * HALF_ROOT, (b[1] + b[3]) * HALF_ROOT
    return (
        (even + odd, even - odd),
        (b[0] + less, b[2] + more),
        (a[0] - a[2], a[1] - a[3]),
        (b[0] - less, more - b[2]),
    )


def butterflies_back(pairs):
    (c0, c4), (c1, s1), (c2, s2), (c3, s3) = pairs
    even, odd = c0 + c4, c0 - c4
    less, more = (c1 - c3) * HALF_ROOT, (s1 + s3) * HALF_ROOT
    a = [even + c2, odd + s2, even - c2, odd - s2]
    b = [c1 + c3, less + more, s1 - s3, more - less]
    return [a[i] + b[i] for i in range(4)] + [a[i] - b[i] for i in range(4)]


def total(block):
    return jnp.sum(jnp.sum(block, axis=0, keepdims=True), axis=1, keepdims=True)


def matmul3(value, high_ref, rest_ref, pair, contract):
    high = value.astype(jnp.bfloat16)
    rest = (value - high.astype(jnp.float32)).astype(jnp.bfloat16)
    dot = functools.partial(
        lax.dot_general,
        dimension_numbers=(((1,), (contract,)), ((), ())),
        preferred_element_type=jnp.float32,
    )
    return dot(high, high_ref[pair]) + (dot(rest, high_ref[pair]) + dot(high, rest_ref[pair]))


class Layout:
    def __init__(self, size, ref):
        self.groups, self.fields, width = ref.shape
        self.size = size
        self.planes = width // (size * size)

    def place(self, group, plane, block):
        start = (plane * RADIX + block) * LANES
        return group, slice(None), slice(start, start + LANES)

    def rows(self, group, plane):
        return pl.ds(pl.multiple_of((group * self.planes + plane) * self.fields, 8), self.fields)

    def over_planes(self, step, *sums):
        zero = jnp.zeros((self.fields, LANES), jnp.float32)

        def run(group, carry):
            for plane in range(self.planes):
                carry = step(group, plane, carry)
            return carry

        return [total(part) for part in lax.fori_loop(0, self.groups, run, (zero,) * len(sums))]

    def spread(self, left, group, plane, values):
        for pair, halves in enumerate(butterflies(values)):
            for half, value in enumerate(halves):
                left[pair, self.rows(group, plane), half * LANES : (half + 1) * LANES] = value

    def collect(self, right, group, plane):
        rows = self.rows(group, plane)
        return butterflies_back(
            [
                [right[pair, rows, half * LANES : (half + 1) * LANES] for half in range(2)]
                for pair in range(PAIRS)
            ]
        )

    def middle(self, left, right, pot_ref, high_ref, rest_ref):
        size, fields = self.size, self.fields

        def into(pair):
            right[pair] = matmul3(left[pair], high_ref, rest_ref, pair, 0)

        def weigh(pair):
            for half in range(2):
                lanes = slice(half * LANES, (half + 1) * LANES)
                column = [right[pair, x * fields : (x + 1) * fields, lanes] for x in range(size)]
                column = hartley(column)
                column = [column[x] * pot_ref[pair, x : x + 1, lanes] for x in range(size)]
                column = hartley(column)
                for x in range(size):
                    left[pair, x * fields : (x + 1) * fields, lanes] = column[x]

        def out(pair):
            right[pair] = matmul3(left[pair], high_ref, rest_ref, pair, 1)

        for stage in range(PAIRS + 2):
            if stage < PAIRS:
                into(stage)
            if 0 <= stage - 2:
                out(stage - 2)
            if 0 <= stage - 1 < PAIRS:
                weigh(stage - 1)


def tree_sum(values):
    while len(values) > 1:
        values = [sum(values[i : i + 2]) for i in range(0, len(values), 2)]
    return values[0]


def inverse_of(value):
    positive = value > 0.0
    return jnp.where(positive, 1.0 / jnp.where(positive, value, 1.0), 0.0)


def first_kernel(
    size, start_ref, pot_ref, high_ref, rest_ref, direct_ref, square_ref, left, right
):
    layout = Layout(size, start_ref)

    def forward(group, plane, carry):
        values = [start_ref[layout.place(group, plane, block)] for block in range(RADIX)]
        layout.spread(left, group, plane, values)
        return (carry[0] + tree_sum([value * value for value in values]),)

    (square,) = layout.over_planes(forward, 0)
    square_ref[...] = jnp.broadcast_to(square, square_ref.shape)
    layout.middle(left, right, pot_ref, high_ref, rest_ref)

    def backward(group, plane, carry):
        for block, direct in enumerate(layout.collect(right, group, plane)):
            direct_ref[layout.place(group, plane, block)] = direct
        return carry

    layout.over_planes(backward)


def recur_kernel(
    size, start_ref, direct_ref, square_ref, energy_ref, pot_ref, high_ref, rest_ref,
    basis_1, basis_2, basis_3, basis_4, message_ref, own_ref, left, right,
):
    layout = Layout(size, start_ref)
    basis = [start_ref, basis_1, basis_2, basis_3, basis_4]
    squares = [square_ref[0:1, 0:1]]
    alphas, betas, lengths = [], [], []

    def remainder(step, group, plane):
        places = [layout.place(group, plane, block) for block in range(RADIX)]
        alpha, scale = alphas[step - 1], inverse_of(lengths[step - 1])
        applied = [basis[step][place] for place in places]
        before = [basis[step - 1][place] for place in places]
        values = [(new - alpha * old) * scale for new, old in zip(applied, before)]
        for place, value in zip(places, values):
            basis[step][place] = value
        return values, tree_sum([value * value for value in values])

    for step in range(ITERS):
        if step > 0:

            def forward(group, plane, carry, step=step):
                values, part = remainder(step, group, plane)
                layout.spread(left, group, plane, values)
                return (carry[0] + part,)

            squares += layout.over_planes(forward, 0)
            layout.middle(left, right, pot_ref, high_ref, rest_ref)
            back = squares[step] * inverse_of(squares[step - 1]) * lengths[step - 1]

        def backward(group, plane, carry, step=step):
            places = [layout.place(group, plane, block) for block in range(RADIX)]
            if step == 0:
                directs = [direct_ref[place] for place in places]
            else:
                olds = [basis[step - 1][place] for place in places]
                directs = layout.collect(right, group, plane)
                directs = [direct + back * old for direct, old in zip(directs, olds)]
            values = [basis[step][place] for place in places]
            applied = [
                energy_ref[place] * value - direct
                for place, value, direct in zip(places, values, directs)
            ]
            for place, new in zip(places, applied):
                basis[step + 1][place] = new
            return (
                carry[0] + tree_sum([value * new for value, new in zip(values, applied)]),
                carry[1] + tree_sum([new * new for new in applied]),
            )

        along, whole = layout.over_planes(backward, 0, 0)
        inverse = inverse_of(squares[step])
        alpha, whole = along * inverse, whole * inverse
        alphas.append(alpha)
        lengths.append(jnp.sqrt(jnp.maximum(whole - alpha * alpha, 1e-6 * whole)))

    def last(group, plane, carry):
        return (carry[0] + remainder(ITERS, group, plane)[1],)

    squares += layout.over_planes(last, 0)
    for step in range(ITERS):
        ratio = squares[step + 1] * inverse_of(squares[step])
        betas.append(jnp.sqrt(ratio) * lengths[step])
    norms = [jnp.sqrt(square) for square in squares]
    table = {ROW_NORM: norms[0]}
    for step in range(ITERS):
        table[step], table[ROW_BETA + step] = alphas[step], betas[step]
    lane = lax.broadcasted_iota(jnp.int32, (1, LANES), 1)
    message = jnp.zeros((1, LANES), jnp.float32)
    for place, value in table.items():
        message = jnp.where(lane == place, value, message)
    message_ref[...] = jnp.broadcast_to(message[None], message_ref.shape)
    for step in range(ITERS + 1):
        table[ROW_INVERSE + step] = inverse_of(norms[step])
    row = lax.broadcasted_iota(jnp.int32, (ROWS, LANES), 0)
    own = jnp.zeros((ROWS, LANES), jnp.float32)
    for place, value in table.items():
        own = jnp.where(row == place, value, own)
    own_ref[...] = own


def combine_kernel(
    root_count, all_ref, own_ref, basis_0, basis_1, basis_2, basis_3, basis_4,
    result_ref, alpha_ref, beta_ref,
):
    basis = [basis_0, basis_1, basis_2, basis_3, basis_4]
    groups, fields, width = result_ref.shape
    table = jnp.transpose(all_ref[:, 0, :])
    wide_alpha, wide_beta = table[0:8], table[8:16]
    own_alpha, own_beta = own_ref[0:8], own_ref[8:16]
    norms = table[ROW_NORM : ROW_NORM + 1]
    inverse = 1.0 / jnp.sqrt(total(norms * norms))

    def first(norm, like):
        row = lax.broadcasted_iota(jnp.int32, like.shape, 0)
        return jnp.where(row == 0, norm * inverse, 0.0)

    def apply(diagonal, side, vector):
        return diagonal * vector + side * pltpu.roll(vector, 7, 0) + pltpu.roll(side * vector, 1, 0)

    wide = first(norms, wide_alpha)
    own = first(own_ref[ROW_NORM : ROW_NORM + 1], own_alpha)
    wide_prev, own_prev = jnp.zeros_like(wide), jnp.zeros_like(own)
    beta = jnp.zeros((1, 1), jnp.float32)
    lane = lax.broadcasted_iota(jnp.int32, (1, LANES), 1)
    alphas = jnp.zeros((1, LANES), jnp.float32)
    betas = jnp.zeros((1, LANES), jnp.float32)
    for step in range(ITERS):
        applied = apply(wide_alpha, wide_beta, wide)
        alpha = total(wide * applied)
        remainder = applied - alpha * wide - beta * wide_prev
        own_remainder = apply(own_alpha, own_beta, own) - alpha * own - beta * own_prev
        beta = jnp.sqrt(total(remainder * remainder))
        wide_prev, own_prev = wide, own
        wide, own = remainder / beta, own_remainder / beta
        alphas = jnp.where(lane == step, alpha, alphas)
        betas = jnp.where(lane == step, beta, betas)
    alpha_ref[0] = alphas[:, :ITERS]
    beta_ref[0] = betas[:, :ITERS]
    scales = own_ref[ROW_INVERSE:ROWS]
    factors = [own[i : i + 1] * scales[i : i + 1] * root_count for i in range(ITERS + 1)]

    def run(group, carry):
        for block in range(width // LANES):
            place = (group, slice(None), slice(block * LANES, (block + 1) * LANES))
            result_ref[place] = tree_sum([basis[i][place] * factors[i] for i in range(ITERS + 1)])
        return carry

    lax.fori_loop(0, groups, run, 0)


def shift_axis(part, offset, axis_number):
    length = part.shape[axis_number]
    doubled = jnp.concatenate([part, part], axis=axis_number)
    first_index = (length - offset) % length
    return lax.dynamic_slice_in_dim(doubled, first_index, length, axis_number)


def potential_table(potential, sites):
    size = potential.shape[0]
    table = potential
    for axis in range(3):
        table = shift_axis(table, sites[axis, 0], axis)
    table = table * (1.0 / size**3)
    table = table.reshape(size, size // RADIX, RADIX, size)
    pairs = [
        jnp.concatenate([table[:, :, residue].reshape(size, -1) for residue in residues], axis=1)
        for residues in RESIDUES
    ]
    return jnp.stack(pairs)


def body(start, energies, sites, potential):
    size = potential.shape[0]
    atom_count, core_count, pol_count, band_local, kpoint_local = start.shape
    assert atom_count == 1 and pol_count == 1 and size * (size // RADIX) == LANES
    groups = lax.axis_size("grid")
    devices = groups * lax.axis_size("band")
    chain = core_count * band_local
    planes = size // groups
    fields = -(-chain // groups)
    padded = -(-fields // 8) * 8

    def by_owner(part):
        part = part.reshape(chain, kpoint_local)
        if fields * groups != chain:
            part = jnp.pad(part, ((0, fields * groups - chain), (0, 0)))
        part = part.reshape(groups, fields, kpoint_local)
        if padded != fields:
            part = jnp.pad(part, ((0, 0), (0, padded - fields), (0, 0)))
        return part

    move = functools.partial(lax.all_to_all, split_axis=0, concat_axis=0, tiled=True)
    own_start = move(by_owner(start), "grid")
    own_energies = move(by_owner(energies), "grid")
    table = potential_table(potential, sites)
    high, rest = map(jnp.asarray, split_weights(pair_weights(size)))
    vmem = pl.BlockSpec(memory_space=pltpu.VMEM)
    shape = functools.partial(jax.ShapeDtypeStruct, dtype=jnp.float32)
    vector = shape((groups, padded, kpoint_local))
    scratch = pltpu.VMEM((PAIRS, size * padded, 2 * LANES), jnp.float32)

    def call(kernel, name, inputs, outputs, scratches, limit):
        return pl.pallas_call(
            kernel,
            out_shape=outputs,
            in_specs=[vmem] * len(inputs),
            out_specs=(vmem,) * len(outputs),
            scratch_shapes=scratches,
            compiler_params=pltpu.CompilerParams(vmem_limit_bytes=limit * 2**20),
            name=name,
        )(*inputs)

    direct, square = call(
        functools.partial(first_kernel, size),
        "first",
        (own_start, table, high, rest),
        (vector, shape((8, LANES))),
        [scratch] * 2,
        16,
    )
    *basis, message, own = call(
        functools.partial(recur_kernel, size),
        "recur",
        (own_start, direct, square, own_energies, table, high, rest),
        (vector,) * ITERS + (shape((devices, 1, LANES)), shape((ROWS, LANES))),
        [scratch] * 2,
        20,
    )
    gathered = move(message, ("grid", "band"))
    count = chain * lax.axis_size("band") * kpoint_local * groups
    result, alphas, betas = call(
        functools.partial(combine_kernel, math.sqrt(count)),
        "combine",
        (gathered, own, own_start, *basis),
        (vector, shape((1, 1, ITERS)), shape((1, 1, ITERS))),
        [],
        16,
    )
    back = move(result, "grid")
    back = back[:, :fields].reshape(groups * fields, kpoint_local)[:chain]
    return alphas, betas, back.reshape(start.shape)


def solution(mesh):
    in_specs = (P(None, None, None, "band", "grid"), P(None, "band", "grid"), P(), P())
    out_specs = (P(), P(), P(None, None, None, "band", "grid"))
    return jax.shard_map(body, mesh=mesh, in_specs=in_specs, out_specs=out_specs, check_vma=False)
```

```python
import functools
import math

import jax
import jax.numpy as jnp
import numpy as np
from jax import lax
from jax.experimental import pallas as pl
from jax.experimental.pallas import tpu as pltpu
from jax.sharding import PartitionSpec as P

ITERS = 4
LANES = 128
RADIX = 8
PAIRS = 4
RESIDUES = ((0, 4), (1, 7), (2, 6), (3, 5))
HALF_ROOT = math.sqrt(0.5)
ROW_BETA = 8
ROW_NORM = 16
ROW_INVERSE = 17
ROWS = 24


def cas(angle):
    return np.cos(angle) + np.sin(angle)


@functools.cache
def pair_weights(size):
    low = size // RADIX
    cells = np.arange(size)
    over_z = cas(2 * np.pi * np.outer(cells, cells) / size)
    weights = np.zeros((PAIRS, 2, low, size, 2, low, size))
    for pair, residues in enumerate(RESIDUES):
        for out_half, residue in enumerate(residues):
            for v0 in range(low):
                for y0 in range(low):
                    angle = 2 * np.pi * (residue + RADIX * v0) * y0 / size
                    cosine, sine = np.cos(angle), np.sin(angle)
                    if pair == 0:
                        weights[pair, out_half, y0, :, out_half, v0] = (cosine + sine) * over_z
                    else:
                        sign = 1.0 if out_half == 0 else -1.0
                        weights[pair, 0, y0, :, out_half, v0] = (cosine + sine) * over_z
                        weights[pair, 1, y0, :, out_half, v0] = sign * (cosine - sine) * over_z
    return weights.reshape(PAIRS, 2 * low * size, 2 * low * size)


def split_weights(weights):
    high = weights.astype(np.float32).astype(jnp.bfloat16)
    rest = (weights - high.astype(np.float64)).astype(np.float32).astype(jnp.bfloat16)
    return high, rest


def hartley(values):
    count = len(values)
    if count == 2:
        return [values[0] + values[1], values[0] - values[1]]
    even, odd = hartley(values[0::2]), hartley(values[1::2])
    half = count // 2
    first, second = [], []
    for u in range(half):
        angle = 2 * math.pi * u / count
        if u == 0:
            turned = odd[0]
        elif 4 * u == count:
            turned = odd[u]
        elif 8 * u == count:
            turned = (odd[u] + odd[half - u]) * HALF_ROOT
        elif 8 * u == 3 * count:
            turned = (odd[half - u] - odd[u]) * HALF_ROOT
        else:
            turned = odd[u] * math.cos(angle) + odd[half - u] * math.sin(angle)
        first.append(even[u] + turned)
        second.append(even[u] - turned)
    return first + second


def butterflies(f):
    a = [f[i] + f[i + 4] for i in range(4)]
    b = [f[i] - f[i + 4] for i in range(4)]
    even, odd = a[0] + a[2], a[1] + a[3]
    less, more = (b[1] - b[3]) * HALF_ROOT, (b[1] + b[3]) * HALF_ROOT
    return (
        (even + odd, even - odd),
        (b[0] + less, b[2] + more),
        (a[0] - a[2], a[1] - a[3]),
        (b[0] - less, more - b[2]),
    )


def butterflies_back(pairs):
    (c0, c4), (c1, s1), (c2, s2), (c3, s3) = pairs
    even, odd = c0 + c4, c0 - c4
    less, more = (c1 - c3) * HALF_ROOT, (s1 + s3) * HALF_ROOT
    a = [even + c2, odd + s2, even - c2, odd - s2]
    b = [c1 + c3, less + more, s1 - s3, more - less]
    return [a[i] + b[i] for i in range(4)] + [a[i] - b[i] for i in range(4)]


def total(block):
    return jnp.sum(jnp.sum(block, axis=0, keepdims=True), axis=1, keepdims=True)


def matmul3(value, high_ref, rest_ref, pair, contract):
    high = value.astype(jnp.bfloat16)
    rest = (value - high.astype(jnp.float32)).astype(jnp.bfloat16)
    dot = functools.partial(
        lax.dot_general,
        dimension_numbers=(((1,), (contract,)), ((), ())),
        preferred_element_type=jnp.float32,
    )
    return dot(high, high_ref[pair]) + (dot(rest, high_ref[pair]) + dot(high, rest_ref[pair]))


class Layout:
    def __init__(self, size, ref):
        self.groups, self.fields, width = ref.shape
        self.size = size
        self.planes = width // (size * size)

    def place(self, group, plane, block):
        start = (plane * RADIX + block) * LANES
        return group, slice(None), slice(start, start + LANES)

    def rows(self, group, plane):
        return pl.ds(pl.multiple_of((group * self.planes + plane) * self.fields, 8), self.fields)

    def over_planes(self, step, *sums):
        zero = jnp.zeros((self.fields, LANES), jnp.float32)

        def run(group, carry):
            for plane in range(self.planes):
                carry = step(group, plane, carry)
            return carry

        return [total(part) for part in lax.fori_loop(0, self.groups, run, (zero,) * len(sums))]

    def spread(self, left, group, plane, values):
        for pair, halves in enumerate(butterflies(values)):
            for half, value in enumerate(halves):
                left[pair, self.rows(group, plane), half * LANES : (half + 1) * LANES] = value

    def collect(self, right, group, plane):
        rows = self.rows(group, plane)
        return butterflies_back(
            [
                [right[pair, rows, half * LANES : (half + 1) * LANES] for half in range(2)]
                for pair in range(PAIRS)
            ]
        )

    def middle(self, left, right, pot_ref, high_ref, rest_ref):
        size, fields = self.size, self.fields

        def into(pair):
            right[pair] = matmul3(left[pair], high_ref, rest_ref, pair, 0)

        def weigh(pair):
            for half in range(2):
                lanes = slice(half * LANES, (half + 1) * LANES)
                column = [right[pair, x * fields : (x + 1) * fields, lanes] for x in range(size)]
                column = hartley(column)
                row = RESIDUES[pair][half]
                column = [column[x] * pot_ref[x, row : row + 1] for x in range(size)]
                column = hartley(column)
                for x in range(size):
                    left[pair, x * fields : (x + 1) * fields, lanes] = column[x]

        def out(pair):
            right[pair] = matmul3(left[pair], high_ref, rest_ref, pair, 1)

        for stage in range(PAIRS + 2):
            if stage < PAIRS:
                into(stage)
            if 0 <= stage - 2:
                out(stage - 2)
            if 0 <= stage - 1 < PAIRS:
                weigh(stage - 1)


def tree_sum(values):
    while len(values) > 1:
        values = [sum(values[i : i + 2]) for i in range(0, len(values), 2)]
    return values[0]


def inverse_of(value):
    positive = value > 0.0
    return jnp.where(positive, 1.0 / jnp.where(positive, value, 1.0), 0.0)


def recur_kernel(
    size, both_ref, pot_ref, high_ref, rest_ref,
    basis_1, basis_2, basis_3, basis_4, message_ref, own_ref, left, right,
):
    layout = Layout(size, basis_1)
    fields = layout.fields
    basis = [both_ref.at[:, :fields], basis_1, basis_2, basis_3, basis_4]
    energy_ref = both_ref.at[:, fields:]
    squares = []
    alphas, betas, lengths = [], [], []

    def remainder(step, group, plane):
        places = [layout.place(group, plane, block) for block in range(RADIX)]
        alpha, scale = alphas[step - 1], inverse_of(lengths[step - 1])
        applied = [basis[step][place] for place in places]
        before = [basis[step - 1][place] for place in places]
        values = [(new - alpha * old) * scale for new, old in zip(applied, before)]
        for place, value in zip(places, values):
            basis[step][place] = value
        return values, tree_sum([value * value for value in values])

    for step in range(ITERS):

        def forward(group, plane, carry, step=step):
            if step == 0:
                values = [basis[0][layout.place(group, plane, block)] for block in range(RADIX)]
                part = tree_sum([value * value for value in values])
            else:
                values, part = remainder(step, group, plane)
            layout.spread(left, group, plane, values)
            return (carry[0] + part,)

        squares += layout.over_planes(forward, 0)
        layout.middle(left, right, pot_ref, high_ref, rest_ref)
        if step > 0:
            back = squares[step] * inverse_of(squares[step - 1]) * lengths[step - 1]

        def backward(group, plane, carry, step=step):
            places = [layout.place(group, plane, block) for block in range(RADIX)]
            directs = layout.collect(right, group, plane)
            if step > 0:
                olds = [basis[step - 1][place] for place in places]
                directs = [direct + back * old for direct, old in zip(directs, olds)]
            values = [basis[step][place] for place in places]
            applied = [
                energy_ref[place] * value - direct
                for place, value, direct in zip(places, values, directs)
            ]
            for place, new in zip(places, applied):
                basis[step + 1][place] = new
            return (
                carry[0] + tree_sum([value * new for value, new in zip(values, applied)]),
                carry[1] + tree_sum([new * new for new in applied]),
            )

        along, whole = layout.over_planes(backward, 0, 0)
        inverse = inverse_of(squares[step])
        alpha, whole = along * inverse, whole * inverse
        alphas.append(alpha)
        lengths.append(jnp.sqrt(jnp.maximum(whole - alpha * alpha, 1e-6 * whole)))

    def last(group, plane, carry):
        return (carry[0] + remainder(ITERS, group, plane)[1],)

    squares += layout.over_planes(last, 0)
    for step in range(ITERS):
        ratio = squares[step + 1] * inverse_of(squares[step])
        betas.append(jnp.sqrt(ratio) * lengths[step])
    norms = [jnp.sqrt(square) for square in squares]
    table = {ROW_NORM: norms[0]}
    for step in range(ITERS):
        table[step], table[ROW_BETA + step] = alphas[step], betas[step]
    lane = lax.broadcasted_iota(jnp.int32, (1, LANES), 1)
    message = jnp.zeros((1, LANES), jnp.float32)
    for place, value in table.items():
        message = jnp.where(lane == place, value, message)
    message_ref[...] = jnp.broadcast_to(message[None], message_ref.shape)
    for step in range(ITERS + 1):
        table[ROW_INVERSE + step] = inverse_of(norms[step])
    row = lax.broadcasted_iota(jnp.int32, (ROWS, LANES), 0)
    own = jnp.zeros((ROWS, LANES), jnp.float32)
    for place, value in table.items():
        own = jnp.where(row == place, value, own)
    own_ref[...] = own


def combine_kernel(
    root_count, all_ref, own_ref, both_ref, basis_1, basis_2, basis_3, basis_4,
    result_ref, alpha_ref, beta_ref,
):
    groups, fields, width = result_ref.shape
    basis = [both_ref.at[:, :fields], basis_1, basis_2, basis_3, basis_4]
    table = jnp.transpose(all_ref[:, 0, :])
    wide_alpha, wide_beta = table[0:8], table[8:16]
    own_alpha, own_beta = own_ref[0:8], own_ref[8:16]
    norms = table[ROW_NORM : ROW_NORM + 1]
    inverse = 1.0 / jnp.sqrt(total(norms * norms))

    def first(norm, like):
        row = lax.broadcasted_iota(jnp.int32, like.shape, 0)
        return jnp.where(row == 0, norm * inverse, 0.0)

    def apply(diagonal, side, vector):
        return diagonal * vector + side * pltpu.roll(vector, 7, 0) + pltpu.roll(side * vector, 1, 0)

    wide = first(norms, wide_alpha)
    own = first(own_ref[ROW_NORM : ROW_NORM + 1], own_alpha)
    wide_prev, own_prev = jnp.zeros_like(wide), jnp.zeros_like(own)
    beta = jnp.zeros((1, 1), jnp.float32)
    lane = lax.broadcasted_iota(jnp.int32, (1, LANES), 1)
    alphas = jnp.zeros((1, LANES), jnp.float32)
    betas = jnp.zeros((1, LANES), jnp.float32)
    for step in range(ITERS):
        applied = apply(wide_alpha, wide_beta, wide)
        alpha = total(wide * applied)
        remainder = applied - alpha * wide - beta * wide_prev
        own_remainder = apply(own_alpha, own_beta, own) - alpha * own - beta * own_prev
        beta = jnp.sqrt(total(remainder * remainder))
        wide_prev, own_prev = wide, own
        wide, own = remainder / beta, own_remainder / beta
        alphas = jnp.where(lane == step, alpha, alphas)
        betas = jnp.where(lane == step, beta, betas)
    alpha_ref[0] = alphas[:, :ITERS]
    beta_ref[0] = betas[:, :ITERS]
    scales = own_ref[ROW_INVERSE:ROWS]
    factors = [own[i : i + 1] * scales[i : i + 1] * root_count for i in range(ITERS + 1)]

    def run(group, carry):
        for block in range(width // LANES):
            place = (group, slice(None), slice(block * LANES, (block + 1) * LANES))
            result_ref[place] = tree_sum([basis[i][place] * factors[i] for i in range(ITERS + 1)])
        return carry

    lax.fori_loop(0, groups, run, 0)


def shift_axis(part, offset, axis_number):
    length = part.shape[axis_number]
    doubled = jnp.concatenate([part, part], axis=axis_number)
    first_index = (length - offset) % length
    return lax.dynamic_slice_in_dim(doubled, first_index, length, axis_number)


def potential_table(potential, sites):
    size = potential.shape[0]
    table = potential
    for axis in range(3):
        table = shift_axis(table, sites[axis, 0], axis)
    table = table * (1.0 / size**3)
    table = table.reshape(size, size // RADIX, RADIX, size)
    return table.transpose(0, 2, 1, 3).reshape(size, RADIX, LANES)


def body(start, energies, sites, potential):
    size = potential.shape[0]
    atom_count, core_count, pol_count, band_local, kpoint_local = start.shape
    assert atom_count == 1 and pol_count == 1 and size * (size // RADIX) == LANES
    groups = lax.axis_size("grid")
    devices = groups * lax.axis_size("band")
    chain = core_count * band_local
    planes = size // groups
    fields = -(-chain // groups)
    padded = -(-fields // 8) * 8

    def by_owner(part):
        part = part.reshape(chain, kpoint_local)
        if fields * groups != chain:
            part = jnp.pad(part, ((0, fields * groups - chain), (0, 0)))
        part = part.reshape(groups, fields, kpoint_local)
        if padded != fields:
            part = jnp.pad(part, ((0, 0), (0, padded - fields), (0, 0)))
        return part

    move = functools.partial(lax.all_to_all, split_axis=0, concat_axis=0, tiled=True)
    both = move(jnp.concatenate([by_owner(start), by_owner(energies)], axis=1), "grid")
    table = potential_table(potential, sites)
    high, rest = map(jnp.asarray, split_weights(pair_weights(size)))
    vmem = pl.BlockSpec(memory_space=pltpu.VMEM)
    shape = functools.partial(jax.ShapeDtypeStruct, dtype=jnp.float32)
    vector = shape((groups, padded, kpoint_local))
    scratch = pltpu.VMEM((PAIRS, size * padded, 2 * LANES), jnp.float32)

    def call(kernel, name, inputs, outputs, scratches, limit):
        return pl.pallas_call(
            kernel,
            out_shape=outputs,
            in_specs=[vmem] * len(inputs),
            out_specs=(vmem,) * len(outputs),
            scratch_shapes=scratches,
            compiler_params=pltpu.CompilerParams(vmem_limit_bytes=limit * 2**20),
            name=name,
        )(*inputs)

    *basis, message, own = call(
        functools.partial(recur_kernel, size),
        "recur",
        (both, table, high, rest),
        (vector,) * ITERS + (shape((devices, 1, LANES)), shape((ROWS, LANES))),
        [scratch] * 2,
        20,
    )
    gathered = move(message, ("grid", "band"))
    count = chain * lax.axis_size("band") * kpoint_local * groups
    result, alphas, betas = call(
        functools.partial(combine_kernel, math.sqrt(count)),
        "combine",
        (gathered, own, both, *basis),
        (vector, shape((1, 1, ITERS)), shape((1, 1, ITERS))),
        [],
        16,
    )
    back = move(result, "grid")
    back = back[:, :fields].reshape(groups * fields, kpoint_local)[:chain]
    return alphas, betas, back.reshape(start.shape)


def solution(mesh):
    in_specs = (P(None, None, None, "band", "grid"), P(None, "band", "grid"), P(), P())
    out_specs = (P(), P(), P(None, None, None, "band", "grid"))
    return jax.shard_map(body, mesh=mesh, in_specs=in_specs, out_specs=out_specs, check_vma=False)
```
